32 devices in a mesh: batch: 1 (over z), row: 4 (over y), col: 8 (over x, core).
Axes of the slice: x: 4, y: 4, z: 1, core: 2. Of those that a mesh axis runs over, the one named last changes fastest.
The devices are a block of a 4x4x8 slice.
Arguments:
- tri_mat: bfloat16 [12288, 12288], P(('batch', 'row'), 'col')
- rhs_mat: bfloat16 [12288, 16384], P(('batch', 'row'), 'col')
Outputs:
- output: bfloat16 [12288, 16384], P(('batch', 'row'), 'col')
All inputs are finite; a program needn't handle non-finite values.
Results may differ from the reference program's by a relative error of at most 0.001.
Values are sent between devices in bfloat16 or wider.
A program may use at most 768 MiB of HBM per device.

```python
import jax
import jax.numpy as jnp

MAT_ORDER = 12288
BLOCK_SIZE = 256
COLS_DEV = 2048
GRID_ROWS = 4
GRID_COLS = 8
NUM_COLS = COLS_DEV * GRID_COLS
NUM_BLOCKS = MAT_ORDER // BLOCK_SIZE


def logical_index(grid_size):
    stored = jnp.arange(MAT_ORDER, dtype=jnp.int32)
    block_idx = stored // BLOCK_SIZE
    per_device = NUM_BLOCKS // grid_size
    owner_dev = block_idx // per_device
    local_blk = block_idx % per_device
    return (local_blk * grid_size + owner_dev) * BLOCK_SIZE + stored % BLOCK_SIZE


def setup_inputs(seed: int = 0, part: int = 0) -> dict:
    base_key = jax.random.fold_in(jax.random.key(seed), part)
    key_tri, key_rhs = jax.random.split(base_key)
    row_ids = logical_index(GRID_ROWS)
    col_ids = logical_index(GRID_COLS)
    lower_mask = row_ids[:, None] >= col_ids[None, :]
    scale_tri = MAT_ORDER ** -0.5
    draws = jax.random.normal(key_tri, (MAT_ORDER, MAT_ORDER), jnp.float32) * scale_tri
    tri_mat = jnp.where(lower_mask, draws, 0.0).astype(jnp.bfloat16)
    rhs_mat = jax.random.normal(key_rhs, (MAT_ORDER, NUM_COLS), jnp.float32).astype(jnp.bfloat16)
    return {"tri_mat": tri_mat, "rhs_mat": rhs_mat}


def reference(tri_mat, rhs_mat):
    by_rows = rhs_mat.reshape(GRID_ROWS, NUM_BLOCKS // GRID_ROWS, BLOCK_SIZE, NUM_COLS)
    logical = by_rows.transpose(1, 0, 2, 3).reshape(NUM_BLOCKS // GRID_COLS, GRID_COLS, BLOCK_SIZE, NUM_COLS)
    rhs_by_cols = logical.transpose(1, 0, 2, 3).reshape(MAT_ORDER, NUM_COLS)
    product = jnp.dot(tri_mat, rhs_by_cols, preferred_element_type=jnp.float32)
    return product.astype(jnp.bfloat16)
```

```python
import functools

import jax
import jax.numpy as jnp
from jax import lax
from jax.experimental import pallas as pl
from jax.experimental.pallas import tpu as pltpu
from jax.sharding import PartitionSpec as P

BLOCK_SIZE = 256
TILE = 256
NUM_WIDE = 4
MESH = pl.DeviceIdType.MESH

PANELS = ((0, 0), (0, 1), (0, 2), (0, 3), (1, 2), (1, 3), (0, 4), (1, 4), (0, 5), (1, 5))
PART_B = ((-1, 0), (-1, 0), (0, 1), (1, 0), (1, 1), (2, 1), (3, 1), (4, 1), (6, 1), (8, 1))
PART_C = ((0, 0), (0, 1), (1, 1), (2, 0), (3, 0), (4, 0), (5, 1), (7, 0), (9, 1), (10, 0))


def kernel(bs, tile, tri, rhs, out, bg, lg, lbuf, bbuf, acc, obuf, lsem, bsem, osem,
           b_send, b_recv, w_send, w_recv, t_send, t_recv, x_send, x_recv, d_send, d_recv,
           o_send, o_recv):
    groups = rhs.shape[0] // bs
    half = rhs.shape[1] // 2
    grid_rows = bg.shape[0]
    grid_cols = lg.shape[1]
    y = lax.axis_index("row")
    q = lax.axis_index("col")
    mate = y + 1 - 2 * lax.rem(y, 2)
    peer = grid_rows - 1 - y
    far = grid_rows - 1 - mate
    mine = lax.rem((y + 1) // 2 + 1, 2)
    q_up = lax.rem(q + 2, grid_cols)
    q_down = lax.rem(q + grid_cols - 2, grid_cols)
    q_far = lax.rem(q + grid_cols // 2, grid_cols)
    q_twin = q + 1 - 2 * lax.rem(q, 2)

    def send(src, dst, ss, rs, **where):
        return pltpu.make_async_remote_copy(src_ref=src, dst_ref=dst, send_sem=ss, recv_sem=rs,
                                            device_id=where, device_id_type=MESH)

    def landed(ref, sem):
        pltpu.make_async_copy(ref, ref, sem).wait()

    def cols_of(side):
        return pl.ds(pl.multiple_of(side * half, half), half)

    def rows_of(j, count=1):
        return pl.ds(pl.multiple_of(j * bs, bs), count * bs)

    def b_copy(kind, j, wide):
        sems = (w_send, w_recv) if wide else (b_send, b_recv)
        side = (mine if kind == 0 else 1 - mine) if wide else (1 - mine if kind == 0 else mine)
        part = (rows_of(j), cols_of(side))
        src = bg.at[(mate, *part)] if kind == 2 else rhs.at[part]
        dst = bg.at[(mate if kind == 2 else y, *part)]
        return send(src, dst, sems[0].at[kind, j], sems[1].at[kind, j], row=mate if kind == 0 else peer)

    def b_landed(kind, j, wide):
        owner = (mate, peer, far)[kind]
        sem = w_recv if wide else b_recv
        landed(bg.at[owner, rows_of(j), cols_of(1 - mine if wide else mine)], sem.at[kind, j])

    def both(j, act):
        act(False)
        if isinstance(j, int):
            if j < NUM_WIDE:
                act(True)
        else:
            @pl.when(j < NUM_WIDE)
            def _():
                act(True)

    def panel(m):
        return rows_of(2 * m, 2), pl.ds(0, (m + 1) * bs)

    def tri_copy(m):
        t = m - NUM_WIDE // 2
        part = panel(m)
        return send(tri.at[part], lg.at[(1, q, *part)], t_send.at[t], t_recv.at[t], row=mate)

    def l_own(n):
        cls, m = PANELS[n]
        return lg.at[(1, q, *panel(m))] if cls else tri.at[panel(m)]

    def l_copy(n, way):
        cls, m = PANELS[n]
        sems = x_send.at[n, way], x_recv.at[n, way]
        if way < 2:
            return send(l_own(n), lg.at[(cls, q, *panel(m))], *sems, col=q_down if way else q_up)
        owner = q_up if way == 3 else q_down
        part = lg.at[cls, owner, rows_of(2 * m + way - 2), pl.ds(0, (m + 1) * bs)]
        return send(part, part, *sems, col=q_down if way == 3 else q_up)

    def twin_copy(n, way):
        cls, m = PANELS[n]
        owner = (q, q_down, q_up, q_far)[way]
        dst = lg.at[(cls, owner, *panel(m))]
        src = l_own(n) if way == 0 else dst
        return send(src, dst, d_send.at[n, way], d_recv.at[n, way], col=q_twin)

    def part_a(n):
        cls, m = PANELS[n]
        if cls:
            landed(lg.at[(1, q, *panel(m))], t_recv.at[m - NUM_WIDE // 2])
        for way in range(2):
            l_copy(n, way).start()
        twin_copy(n, 0).start()

    def part_b(n):
        cls, m = PANELS[n]
        for way, owner in enumerate((q_down, q_up)):
            landed(lg.at[(cls, owner, *panel(m))], x_recv.at[n, way])
            l_copy(n, 2 + way).start()
        for way in range(2):
            twin_copy(n, 1 + way).start()
        if n + 2 < len(PANELS):
            part_a(n + 2)

    def part_c(n):
        cls, m = PANELS[n]
        for way in range(2):
            half_panel = lg.at[cls, q_far, rows_of(2 * m + way), pl.ds(0, (m + 1) * bs)]
            landed(half_panel, x_recv.at[n, 2 + way])
        twin_copy(n, 3).start()

    def part_d(n):
        cls, m = PANELS[n]
        for way, owner in enumerate((q, q_down, q_up, q_far)):
            twin = owner + 1 - 2 * lax.rem(owner, 2)
            landed(lg.at[(cls, twin, *panel(m))], d_recv.at[n, way])

    def events(j, pos, lo, hi):
        for n in range(len(PANELS)):
            for spots, part in ((PART_C, part_c), (PART_B, part_b)):
                if spots[n][1] == pos and lo <= spots[n][0] < hi:
                    pl.when(j == spots[n][0])(functools.partial(part, n))
        if pos == 0:
            for n, (_, m) in enumerate(PANELS):
                if lo <= 2 * m < hi:
                    pl.when(j == 2 * m)(functools.partial(part_d, n))

    def fetch_l(j, g, slot, wide):
        spot = rows_of(j), rows_of(g // 2)
        for p in range(4):
            owner = 4 * lax.rem(g, 2) + p
            dst = lbuf.at[slot, pl.ds(0, bs), pl.ds(p * bs, bs)]

            @pl.when(owner == q)
            def _():
                pltpu.make_async_copy(tri.at[spot], dst, lsem.at[slot]).start()

            @pl.when(owner != q)
            def _():
                pltpu.make_async_copy(lg.at[(0, owner, *spot)], dst, lsem.at[slot]).start()

            if not wide:
                dst = lbuf.at[slot, pl.ds(bs, bs), pl.ds(p * bs, bs)]
                pltpu.make_async_copy(lg.at[(1, owner, *spot)], dst, lsem.at[slot]).start()

    def fetch_b(g, slot, wide):
        for side in range(2 if wide else 1):
            spot = rows_of(g), cols_of(side if wide else mine)
            for p in range(4):
                dst = bbuf.at[slot, side, pl.ds(p * bs, bs), :]

                @pl.when(p == y)
                def _():
                    pltpu.make_async_copy(rhs.at[spot], dst, bsem.at[slot]).start()

                @pl.when(p != y)
                def _():
                    pltpu.make_async_copy(bg.at[(p, *spot)], dst, bsem.at[slot]).start()

    def fetched(slot, wide):
        l_part = lbuf.at[slot, pl.ds(0, bs)] if wide else lbuf.at[slot]
        b_part = bbuf.at[slot] if wide else bbuf.at[slot, 0]
        landed(l_part, lsem.at[slot])
        landed(b_part, bsem.at[slot])

    tiles = half // tile

    def multiply(slot, wide):
        if wide:
            @pl.loop(0, 2 * tiles)
            def _(n):
                side = n // tiles
                cols = pl.ds(pl.multiple_of(lax.rem(n, tiles) * tile, tile), tile)
                rows = rows_of(side)
                acc[rows, cols] += jnp.dot(lbuf[slot, pl.ds(0, bs), :], bbuf[slot, side, :, cols],
                                           preferred_element_type=jnp.float32)
        else:
            @pl.loop(0, tiles)
            def _(n):
                cols = pl.ds(pl.multiple_of(n * tile, tile), tile)
                acc[:, cols] += jnp.dot(lbuf[slot], bbuf[slot, 0, :, cols],
                                        preferred_element_type=jnp.float32)

    def out_copy(j, side):
        return pltpu.make_async_copy(obuf.at[j, pl.ds(side * bs, bs)], out.at[rows_of(j), cols_of(side)],
                                     osem.at[j])

    def own_copy(j):
        return pltpu.make_async_copy(obuf.at[j, pl.ds(0, bs)], out.at[rows_of(j), cols_of(mine)], osem.at[j])

    def mate_copy(j):
        return send(obuf.at[j, pl.ds(bs, bs)], out.at[rows_of(j), cols_of(mine)], o_send.at[j], o_recv.at[j],
                    row=mate)

    def own_block(j):
        both(j, lambda wide: b_copy(1, j, wide).start())
        both(j, lambda wide: b_copy(0, j, wide).start())

    def stage(j, wide, lo, hi):
        for w in ((False, True) if wide else (False,)):
            b_landed(0, j, w)
            b_copy(2, j, w).start()
        if wide:
            for m in range(NUM_WIDE):
                pl.when(j == m)(lambda m=m: tri_copy(m + NUM_WIDE // 2).start())

        @pl.when(j + 2 < groups)
        def _():
            own_block(j + 2)

        events(j, 0, lo, hi)
        acc[...] = jnp.zeros_like(acc)

        @pl.when(j > 0)
        def _():
            fetch_l(j, 0, 0, wide)
            fetch_b(0, 0, wide)

        @pl.loop(0, j)
        def _(g):
            slot = lax.rem(g, 2)
            fetched(slot, wide)
            fetch_l(j, g + 1, 1 - slot, wide)

            @pl.when(g + 1 < j)
            def _():
                fetch_b(g + 1, 1 - slot, wide)

            multiply(slot, wide)

        events(j, 1, lo, hi)
        last = lax.rem(j, 2)

        @pl.when(j == 0)
        def _():
            fetch_l(j, j, last, wide)

        for w in ((False, True) if wide else (False,)):
            b_landed(1, j, w)
            b_landed(2, j, w)
        fetch_b(j, last, wide)
        fetched(last, wide)
        multiply(last, wide)

        @pl.loop(0, tiles)
        def _(n):
            cols = pl.ds(pl.multiple_of(n * tile, tile), tile)
            obuf[j, :, cols] = acc[:, cols].astype(obuf.dtype)

        if wide:
            out_copy(j, 0).start()
            out_copy(j, 1).start()
        else:
            mate_copy(j).start()
            own_copy(j).start()

    barrier = pltpu.get_barrier_semaphore()
    for where in ({"row": mate}, {"row": peer}, {"col": q_up}, {"col": q_down}, {"col": q_twin}):
        pl.semaphore_signal(barrier, inc=1, device_id=where, device_id_type=MESH)
    pl.semaphore_wait(barrier, 5)

    own_block(0)
    part_a(0)
    own_block(1)
    part_a(1)
    for n in range(len(PANELS)):
        if PART_B[n][0] < 0:
            part_b(n)

    @pl.loop(0, NUM_WIDE)
    def _(j):
        stage(j, True, 0, NUM_WIDE)

    @pl.loop(NUM_WIDE, groups)
    def _(j):
        stage(j, False, NUM_WIDE, groups)

    @pl.loop(0, NUM_WIDE)
    def _(j):
        landed(obuf.at[j], osem.at[j])
        for kind in range(3):
            b_copy(kind, j, True).wait_send()

    @pl.loop(NUM_WIDE, groups)
    def _(j):
        own_copy(j).wait()
        mate_copy(j).wait_send()
        landed(out.at[rows_of(j), cols_of(1 - mine)], o_recv.at[j])

    @pl.loop(0, groups)
    def _(j):
        for kind in range(3):
            b_copy(kind, j, False).wait_send()

    for m in range(NUM_WIDE):
        tri_copy(m + NUM_WIDE // 2).wait_send()
    for n in range(len(PANELS)):
        for way in range(4):
            l_copy(n, way).wait_send()
            twin_copy(n, way).wait_send()


def solution(mesh):
    grid_rows = mesh.shape["row"]
    grid_cols = mesh.shape["col"]
    bs = BLOCK_SIZE

    def local_trmm(tri_loc, rhs_loc):
        rows_loc, cols_loc = rhs_loc.shape
        groups = rows_loc // bs
        half = cols_loc // 2
        dtype = rhs_loc.dtype
        any_spec = pl.BlockSpec(memory_space=pl.ANY)
        dma = pltpu.SemaphoreType.DMA
        panels = len(PANELS)
        res = pl.pallas_call(
            functools.partial(kernel, bs, min(TILE, half)),
            out_shape=[
                jax.ShapeDtypeStruct((rows_loc, cols_loc), dtype),
                jax.ShapeDtypeStruct((grid_rows, rows_loc, cols_loc), dtype),
                jax.ShapeDtypeStruct((2, grid_cols, *tri_loc.shape), dtype),
            ],
            in_specs=[any_spec] * 2,
            out_specs=[any_spec] * 3,
            scratch_shapes=[
                pltpu.VMEM((2, 2 * bs, 4 * bs), dtype),
                pltpu.VMEM((2, 2, 4 * bs, half), dtype),
                pltpu.VMEM((2 * bs, half), jnp.float32),
                pltpu.VMEM((groups, 2 * bs, half), dtype),
                dma((2,)), dma((2,)), dma((groups,)),
                dma((3, groups)), dma((3, groups)),
                dma((3, NUM_WIDE)), dma((3, NUM_WIDE)),
                dma((NUM_WIDE,)), dma((NUM_WIDE,)),
                dma((panels, 4)), dma((panels, 4)),
                dma((panels, 4)), dma((panels, 4)),
                dma((groups,)), dma((groups,)),
            ],
            compiler_params=pltpu.CompilerParams(
                collective_id=0, has_side_effects=True, vmem_limit_bytes=48 * 1024 * 1024),
        )(tri_loc, rhs_loc)
        return res[0]

    part_spec = P(("batch", "row"), "col")
    return jax.shard_map(local_trmm, mesh=mesh, in_specs=(part_spec, part_spec), out_specs=part_spec, check_vma=False)
```

```python
import functools

import jax
import jax.numpy as jnp
from jax import lax
from jax.experimental import pallas as pl
from jax.experimental.pallas import tpu as pltpu
from jax.sharding import PartitionSpec as P

BLOCK_SIZE = 256
TILE = 256
NUM_WIDE = 4
MESH = pl.DeviceIdType.MESH

PANELS = (
    (0, 0, 2), (0, 2, 2), (0, 4, 2), (0, 6, 2), (1, 4, 2), (1, 6, 2), (0, 8, 2),
    (1, 8, 2), (0, 10, 1), (1, 10, 1), (0, 11, 1), (1, 11, 1),
)

SCHEDULE = {
    (-1, 0): ("a3", "p1", "m0", "a0", "m9", "f0", "a2",),
    (0, 0): ("b0", "a1", "m1", "p0", "c0",),
    (0, 1): ("b3", "m2", "f1", "t4", "a6",),
    (1, 0): ("t5", "p2",),
    (1, 1): ("b2",),
    (2, 0): ("b1", "a4", "f2", "c1", "m5", "b6",),
    (2, 1): ("a5", "p3", "m4", "c2", "m3",),
    (3, 0): ("a8", "t7", "f4", "c6", "f3", "m6", "c3",),
    (3, 1): ("f5", "b4", "b5", "t9", "p4",),
    (4, 0): ("p5", "a7", "c4",),
    (4, 1): ("c5", "b8", "m7", "m8",),
    (5, 0): ("p6",),
    (5, 1): ("f6",),
    (6, 0): ("b7", "a9", "p7",),
    (6, 1): ("f7", "t11", "f8",),
    (7, 0): ("a10", "c7", "p8",),
    (8, 0): ("p9", "b9",),
    (8, 1): ("c8", "f9", "a11", "m10",),
    (9, 0): ("c9", "p10", "b10", "m11",),
    (10, 0): ("b11", "f10",),
    (10, 1): ("c11", "c10", "p11", "f11",),
}


def kernel(bs, tile, tri, rhs, out, bg, lg, lbuf, bbuf, acc, obuf, lsem, bsem,
           b_send, b_recv, t_send, t_recv, x_send, x_recv, d_send, d_recv, o_send, o_recv):
    groups = rhs.shape[0] // bs
    last = groups - 1
    half = rhs.shape[1] // 2
    quarter = half // 2
    grid_rows = bg.shape[0]
    grid_cols = lg.shape[1]
    y = lax.axis_index("row")
    q = lax.axis_index("col")
    mate = y + 1 - 2 * lax.rem(y, 2)
    peer = grid_rows - 1 - y
    far = grid_rows - 1 - mate
    mine = lax.rem((y + 1) // 2 + 1, 2)
    q_up = lax.rem(q + 2, grid_cols)
    q_down = lax.rem(q + grid_cols - 2, grid_cols)
    q_far = lax.rem(q + grid_cols // 2, grid_cols)
    q_twin = q + 1 - 2 * lax.rem(q, 2)

    def send(src, dst, ss, rs, **where):
        return pltpu.make_async_remote_copy(src_ref=src, dst_ref=dst, send_sem=ss, recv_sem=rs,
                                            device_id=where, device_id_type=MESH)

    def landed(ref, sem):
        pltpu.make_async_copy(ref, ref, sem).wait()

    def rows_of(j, count=1):
        return pl.ds(pl.multiple_of(j * bs, bs), count * bs)

    def cols_of(side, first=0, width=half):
        return pl.ds(pl.multiple_of(side * half + first, width), width)

    def pieces(j):
        return 2 if j < NUM_WIDE or j == last else 1

    def piece_of(j, part):
        index = 2 * j + part if j < NUM_WIDE else NUM_WIDE + j + part
        if j == last:
            return index, False, part * quarter, quarter
        return index, part == 1, 0, half

    def b_copy(kind, j, part):
        index, other, first, width = piece_of(j, part)
        side = (mine if other else 1 - mine) if kind == 0 else (1 - mine if other else mine)
        spot = (rows_of(j), cols_of(side, first, width))
        src = bg.at[(mate, *spot)] if kind == 2 else rhs.at[spot]
        dst = bg.at[(mate if kind == 2 else y, *spot)]
        return send(src, dst, b_send.at[kind, index], b_recv.at[kind, index], row=mate if kind == 0 else peer)

    def b_landed(kind, rows, cols, index):
        landed(bg.at[(mate, peer, far)[kind], rows, cols], b_recv.at[kind, index])

    def own_b(kind, j):
        for part in range(pieces(j)):
            b_copy(kind, j, part).start()

    def relay_b(j):
        for part in range(pieces(j)):
            index, other, first, width = piece_of(j, part)
            b_landed(0, rows_of(j), cols_of(1 - mine if other else mine, first, width), index)
            b_copy(2, j, part).start()

    def panel(n):
        _, first, count = PANELS[n]
        return rows_of(first, count), pl.ds(0, ((first + count - 1) // 2 + 1) * bs)

    def half_panel(n, part):
        _, first, count = PANELS[n]
        rows = count * bs // 2
        start = pl.multiple_of(first * bs + part * rows, rows)
        return pl.ds(start, rows), pl.ds(0, ((first + count - 1) // 2 + 1) * bs)

    def tri_copy(n):
        return send(tri.at[panel(n)], lg.at[(1, q, *panel(n))], t_send.at[n], t_recv.at[n], row=mate)

    def l_own(n):
        return lg.at[(1, q, *panel(n))] if PANELS[n][0] else tri.at[panel(n)]

    def l_copy(n, way):
        cls = PANELS[n][0]
        sems = x_send.at[n, way], x_recv.at[n, way]
        where = q_up if way in (0, 2) else q_down
        if way < 2:
            return send(l_own(n), lg.at[(cls, q, *panel(n))], *sems, col=where)
        part = lg.at[(cls, q_down if way == 2 else q_up, *half_panel(n, way - 2))]
        return send(part, part, *sems, col=where)

    def twin_copy(n, way):
        cls = PANELS[n][0]
        dst = lg.at[(cls, (q, q_down, q_up, q_far)[way], *panel(n))]
        return send(l_own(n) if way == 0 else dst, dst, d_send.at[n, way], d_recv.at[n, way], col=q_twin)

    def part_a(n):
        if PANELS[n][0]:
            landed(l_own(n), t_recv.at[n])
        for way in range(2):
            l_copy(n, way).start()
        twin_copy(n, 0).start()

    def part_b(n):
        for way, owner in enumerate((q_down, q_up)):
            landed(lg.at[(PANELS[n][0], owner, *panel(n))], x_recv.at[n, way])
            l_copy(n, 2 + way).start()
        for way in range(2):
            twin_copy(n, 1 + way).start()

    def part_c(n):
        for way in range(2):
            landed(lg.at[(PANELS[n][0], q_far, *half_panel(n, way))], x_recv.at[n, 2 + way])
        twin_copy(n, 3).start()

    def part_d(n):
        for way, owner in enumerate((q, q_down, q_up, q_far)):
            twin = owner + 1 - 2 * lax.rem(owner, 2)
            landed(lg.at[(PANELS[n][0], twin, *panel(n))], d_recv.at[n, way])

    steps = {
        "p": functools.partial(own_b, 1), "m": functools.partial(own_b, 0), "f": relay_b,
        "t": lambda n: tri_copy(n).start(), "a": part_a, "b": part_b, "c": part_c,
    }

    def play(group, pos):
        for text in SCHEDULE.get((group, pos), ()):
            steps[text[0]](int(text[1:]))
        if pos == 0:
            for n, (_, first, _) in enumerate(PANELS):
                if first == group:
                    part_d(n)

    def events(j, pos, lo, hi):
        for group in range(lo, hi):
            if SCHEDULE.get((group, pos)) or (pos == 0 and any(p[1] == group for p in PANELS)):
                pl.when(j == group)(functools.partial(play, group, pos))

    def fetch_l(j, g, slot, wide):
        spot = rows_of(j), rows_of(g // 2)
        for p in range(4):
            owner = 4 * lax.rem(g, 2) + p
            dst = lbuf.at[slot, pl.ds(0, bs), pl.ds(p * bs, bs)]

            @pl.when(owner == q)
            def _():
                pltpu.make_async_copy(tri.at[spot], dst, lsem.at[slot]).start()

            @pl.when(owner != q)
            def _():
                pltpu.make_async_copy(lg.at[(0, owner, *spot)], dst, lsem.at[slot]).start()

            if not wide:
                dst = lbuf.at[slot, pl.ds(bs, bs), pl.ds(p * bs, bs)]
                pltpu.make_async_copy(lg.at[(1, owner, *spot)], dst, lsem.at[slot]).start()

    def fetch_block(owner, g, slot, wide, first=0, width=half):
        for side in range(2 if wide else 1):
            spot = rows_of(g), cols_of(side if wide else mine, first, width)
            dst = bbuf.at[slot, side, rows_of(owner), pl.ds(first, width)]

            @pl.when(owner == y)
            def _():
                pltpu.make_async_copy(rhs.at[spot], dst, bsem.at[slot]).start()

            @pl.when(owner != y)
            def _():
                pltpu.make_async_copy(bg.at[(owner, *spot)], dst, bsem.at[slot]).start()

    def fetch_b(g, slot, wide):
        for p in range(4):
            fetch_block(p, g, slot, wide)

    def l_fetched(slot, wide):
        landed(lbuf.at[slot, pl.ds(0, bs)] if wide else lbuf.at[slot], lsem.at[slot])

    def b_fetched(slot, wide):
        landed(bbuf.at[slot] if wide else bbuf.at[slot, 0], bsem.at[slot])

    tiles = half // tile

    def product(slot, n, wide):
        if wide:
            side, cols = n // tiles, pl.ds(pl.multiple_of(lax.rem(n, tiles) * tile, tile), tile)
            rows = rows_of(side)
            left = lbuf[slot, pl.ds(0, bs), :]
        else:
            side, cols = 0, pl.ds(pl.multiple_of(n * tile, tile), tile)
            rows = pl.ds(0, 2 * bs)
            left = lbuf[slot]
        term = jnp.dot(left, bbuf[slot, side, :, cols], preferred_element_type=jnp.float32)
        return rows, cols, acc[rows, cols] + term

    def multiply(slot, wide):
        @pl.loop(0, 2 * tiles if wide else tiles)
        def _(n):
            rows, cols, total = product(slot, n, wide)
            acc[rows, cols] = total

    def finish(j, slot, wide, lo=0, hi=tiles):
        @pl.loop(lo, 2 * tiles if wide else hi)
        def _(n):
            _, _, total = product(slot, n, wide)
            total = total.astype(out.dtype)
            if wide:
                out[rows_of(j), pl.ds(pl.multiple_of(n * tile, tile), tile)] = total
            else:
                cols = pl.ds(pl.multiple_of(n * tile, tile), tile)
                obuf[rows_of(j - NUM_WIDE), cols] = total[bs:]
                cols = pl.ds(pl.multiple_of(mine * half + n * tile, tile), tile)
                out[rows_of(j), cols] = total[:bs]

    def mate_copy(j, index, first=0, width=half):
        return send(obuf.at[rows_of(j - NUM_WIDE), pl.ds(first, width)],
                    out.at[rows_of(j), cols_of(mine, first, width)],
                    o_send.at[index], o_recv.at[index], row=mate)

    def older_terms(j, wide):
        acc[...] = jnp.zeros_like(acc)
        fetch_l(j, 0, 0, wide)
        if not wide:
            fetch_b(0, 0, wide)
        else:
            pl.when(j > 0)(lambda: fetch_b(0, 0, wide))

        @pl.loop(0, j)
        def _(g):
            slot = lax.rem(g, 2)
            l_fetched(slot, wide)
            b_fetched(slot, wide)
            fetch_l(j, g + 1, 1 - slot, wide)

            @pl.when(g + 1 < j)
            def _():
                fetch_b(g + 1, 1 - slot, wide)

            multiply(slot, wide)

    def stage(j, wide, lo, hi):
        events(j, 0, lo, hi)
        older_terms(j, wide)
        events(j, 1, lo, hi)
        slot = lax.rem(j, 2)
        fetch_block(y, j, slot, wide)
        fetch_block(mate, j, slot, wide)
        for kind, owner in ((1, peer), (2, far)):
            if wide:
                b_landed(kind, rows_of(j), cols_of(mine), 2 * j)
                b_landed(kind, rows_of(j), cols_of(1 - mine), 2 * j + 1)
            else:
                b_landed(kind, rows_of(j), cols_of(mine), NUM_WIDE + j)
            fetch_block(owner, j, slot, wide)
        l_fetched(slot, wide)
        b_fetched(slot, wide)
        finish(j, slot, wide)
        if not wide:
            mate_copy(j, j - NUM_WIDE).start()

    barrier = pltpu.get_barrier_semaphore()
    for where in ({"row": mate}, {"row": peer}, {"col": q_up}, {"col": q_down}, {"col": q_twin}):
        pl.semaphore_signal(barrier, inc=1, device_id=where, device_id_type=MESH)
    pl.semaphore_wait(barrier, 5)

    play(-1, 0)

    @pl.loop(0, NUM_WIDE)
    def _(j):
        stage(j, True, 0, NUM_WIDE)

    @pl.loop(NUM_WIDE, last)
    def _(j):
        stage(j, False, NUM_WIDE, last)

    play(last, 0)
    older_terms(last, False)
    play(last, 1)
    slot = last % 2
    l_fetched(slot, False)
    for part in range(2):
        index, _, first, width = piece_of(last, part)
        fetch_block(y, last, slot, False, first, width)
        fetch_block(mate, last, slot, False, first, width)
        for kind, owner in ((1, peer), (2, far)):
            b_landed(kind, rows_of(last), cols_of(mine, first, width), index)
            fetch_block(owner, last, slot, False, first, width)
        landed(bbuf.at[slot, 0, :, pl.ds(first, width)], bsem.at[slot])
        finish(last, slot, False, part * tiles // 2, (part + 1) * tiles // 2)
        mate_copy(last, last - NUM_WIDE + part, first, width).start()

    for j in range(groups):
        for kind in range(3):
            for part in range(pieces(j)):
                b_copy(kind, j, part).wait_send()
    for n in range(len(PANELS)):
        if PANELS[n][0]:
            tri_copy(n).wait_send()
        for way in range(4):
            l_copy(n, way).wait_send()
            twin_copy(n, way).wait_send()

    @pl.loop(NUM_WIDE, last)
    def _(j):
        mate_copy(j, j - NUM_WIDE).wait_send()
        landed(out.at[rows_of(j), cols_of(1 - mine)], o_recv.at[j - NUM_WIDE])

    for part in range(2):
        index, _, first, width = piece_of(last, part)
        mate_copy(last, last - NUM_WIDE + part, first, width).wait_send()
        landed(out.at[rows_of(last), cols_of(1 - mine, first, width)], o_recv.at[last - NUM_WIDE + part])


def emit(parts, src, dst, sem):
    rows = src.shape[0] // parts

    def copy(n):
        spot = pl.ds(n * rows, rows)
        return pltpu.make_async_copy(src.at[spot], dst.at[spot], sem.at[n])

    for n in range(parts):
        copy(n).start()
    for n in range(parts):
        copy(n).wait()


def solution(mesh):
    grid_rows = mesh.shape["row"]
    grid_cols = mesh.shape["col"]
    bs = BLOCK_SIZE

    def local_trmm(tri_loc, rhs_loc):
        rows_loc, cols_loc = rhs_loc.shape
        groups = rows_loc // bs
        half = cols_loc // 2
        dtype = rhs_loc.dtype
        any_spec = pl.BlockSpec(memory_space=pl.ANY)
        vmem_spec = pl.BlockSpec(memory_space=pltpu.VMEM)
        dma = pltpu.SemaphoreType.DMA
        panels = len(PANELS)
        in_vmem, _, _ = pl.pallas_call(
            functools.partial(kernel, bs, min(TILE, half)),
            out_shape=[
                pltpu.VMEM((rows_loc, cols_loc), dtype),
                jax.ShapeDtypeStruct((grid_rows, rows_loc, cols_loc), dtype),
                jax.ShapeDtypeStruct((2, grid_cols, *tri_loc.shape), dtype),
            ],
            in_specs=[any_spec] * 2,
            out_specs=[vmem_spec, any_spec, any_spec],
            scratch_shapes=[
                pltpu.VMEM((2, 2 * bs, 4 * bs), dtype),
                pltpu.VMEM((2, 2, 4 * bs, half), dtype),
                pltpu.VMEM((2 * bs, half), jnp.float32),
                pltpu.VMEM(((groups - NUM_WIDE) * bs, half), dtype),
                dma((2,)), dma((2,)),
                dma((3, groups + NUM_WIDE + 1)), dma((3, groups + NUM_WIDE + 1)),
                dma((panels,)), dma((panels,)),
                dma((panels, 4)), dma((panels, 4)),
                dma((panels, 4)), dma((panels, 4)),
                dma((groups - NUM_WIDE + 1,)), dma((groups - NUM_WIDE + 1,)),
            ],
            compiler_params=pltpu.CompilerParams(
                collective_id=0, has_side_effects=True, vmem_limit_bytes=36 * 1024 * 1024),
        )(tri_loc, rhs_loc)
        return pl.pallas_call(
            functools.partial(emit, groups),
            out_shape=jax.ShapeDtypeStruct((rows_loc, cols_loc), dtype),
            in_specs=[vmem_spec],
            out_specs=any_spec,
            scratch_shapes=[dma((groups,))],
            compiler_params=pltpu.CompilerParams(vmem_limit_bytes=1024 * 1024),
        )(in_vmem)

    part_spec = P(("batch", "row"), "col")
    return jax.shard_map(local_trmm, mesh=mesh, in_specs=(part_spec, part_spec), out_specs=part_spec, check_vma=False)
```

```python
import functools

import jax
import jax.numpy as jnp
from jax import lax
from jax.experimental import pallas as pl
from jax.experimental.pallas import tpu as pltpu
from jax.sharding import PartitionSpec as P

BLOCK_SIZE = 256
TILE = 256
NUM_WIDE = 4
SLOTS = 4
MESH = pl.DeviceIdType.MESH

PANELS = (
    (0, 0, 2), (0, 2, 2), (0, 4, 2), (0, 6, 2), (1, 4, 2), (1, 6, 2), (0, 8, 2),
    (1, 8, 2), (0, 10, 1), (1, 10, 1), (0, 11, 1), (1, 11, 1),
)

SCHEDULE = {
    (-1, 0): ("m0", "p5", "p0", "a0", "a1", "b0", "m1", "a6",),
    (0, 0): ("c0",),
    (0, 1): ("t4", "a2", "f0", "f1", "m9",),
    (1, 0): ("b6", "b2", "m2",),
    (1, 1): ("t5", "a3", "p1", "f2", "b1",),
    (2, 0): ("c2", "b3", "t7", "c1", "p2", "p4", "a4",),
    (2, 1): ("a5", "m4", "b4", "p3", "m3",),
    (3, 0): ("a7",),
    (3, 1): ("c4", "m6", "b5", "c3", "m5", "m8", "f3", "f4", "t9",),
    (4, 0): ("a8", "b7", "p6",),
    (4, 1): ("m7", "f5",),
    (5, 0): ("f6", "c5",),
    (5, 1): ("t11", "c6",),
    (6, 0): ("a9", "a10", "f7",),
    (6, 1): ("p7", "p8", "b8", "f8",),
    (7, 1): ("b9", "m10", "c7",),
    (8, 0): ("p9",),
    (8, 1): ("f9", "c8", "a11", "m11",),
    (9, 0): ("p10", "c9",),
    (9, 1): ("b10",),
    (10, 0): ("f10", "b11",),
    (10, 1): ("c10", "p11", "f11", "c11",),
}


def kernel(bs, tile, tri, rhs, out, bg, lg, lbuf, bbuf, acc, obuf, lsem, bsem,
           b_send, b_recv, t_send, t_recv, x_send, x_recv, d_send, d_recv, o_send, o_recv):
    groups = rhs.shape[0] // bs
    last = groups - 1
    half = rhs.shape[1] // 2
    quarter = half // 2
    grid_rows = bg.shape[0]
    grid_cols = lg.shape[1]
    y = lax.axis_index("row")
    q = lax.axis_index("col")
    mate = y + 1 - 2 * lax.rem(y, 2)
    peer = grid_rows - 1 - y
    far = grid_rows - 1 - mate
    mine = lax.rem((y + 1) // 2 + 1, 2)
    q_up = lax.rem(q + 2, grid_cols)
    q_down = lax.rem(q + grid_cols - 2, grid_cols)
    q_far = lax.rem(q + grid_cols // 2, grid_cols)
    q_twin = q + 1 - 2 * lax.rem(q, 2)

    def send(src, dst, ss, rs, **where):
        return pltpu.make_async_remote_copy(src_ref=src, dst_ref=dst, send_sem=ss, recv_sem=rs,
                                            device_id=where, device_id_type=MESH)

    def landed(ref, sem):
        pltpu.make_async_copy(ref, ref, sem).wait()

    def rows_of(j, count=1):
        return pl.ds(pl.multiple_of(j * bs, bs), count * bs)

    def cols_of(side, first=0, width=half):
        return pl.ds(pl.multiple_of(side * half + first, width), width)

    def pieces(j):
        return 2 if j < NUM_WIDE or j == last else 1

    def piece_of(j, part):
        index = 2 * j + part if j < NUM_WIDE else NUM_WIDE + j + part
        if j == last:
            return index, False, part * quarter, quarter
        return index, part == 1, 0, half

    def b_copy(kind, j, part):
        index, other, first, width = piece_of(j, part)
        side = (mine if other else 1 - mine) if kind == 0 else (1 - mine if other else mine)
        spot = (rows_of(j), cols_of(side, first, width))
        src = bg.at[(mate, *spot)] if kind == 2 else rhs.at[spot]
        dst = bg.at[(mate if kind == 2 else y, *spot)]
        return send(src, dst, b_send.at[kind, index], b_recv.at[kind, index], row=mate if kind == 0 else peer)

    def b_landed(kind, rows, cols, index):
        landed(bg.at[(mate, peer, far)[kind], rows, cols], b_recv.at[kind, index])

    def own_b(kind, j):
        for part in range(pieces(j)):
            b_copy(kind, j, part).start()

    def relay_b(j):
        for part in range(pieces(j)):
            index, other, first, width = piece_of(j, part)
            b_landed(0, rows_of(j), cols_of(1 - mine if other else mine, first, width), index)
            b_copy(2, j, part).start()

    def panel(n):
        _, first, count = PANELS[n]
        return rows_of(first, count), pl.ds(0, ((first + count - 1) // 2 + 1) * bs)

    def half_panel(n, part):
        _, first, count = PANELS[n]
        rows = count * bs // 2
        start = pl.multiple_of(first * bs + part * rows, rows)
        return pl.ds(start, rows), pl.ds(0, ((first + count - 1) // 2 + 1) * bs)

    def tri_copy(n):
        return send(tri.at[panel(n)], lg.at[(1, q, *panel(n))], t_send.at[n], t_recv.at[n], row=mate)

    def l_own(n):
        return lg.at[(1, q, *panel(n))] if PANELS[n][0] else tri.at[panel(n)]

    def l_copy(n, way):
        cls = PANELS[n][0]
        sems = x_send.at[n, way], x_recv.at[n, way]
        where = q_up if way in (0, 2) else q_down
        if way < 2:
            return send(l_own(n), lg.at[(cls, q, *panel(n))], *sems, col=where)
        part = lg.at[(cls, q_down if way == 2 else q_up, *half_panel(n, way - 2))]
        return send(part, part, *sems, col=where)

    def twin_copy(n, way):
        cls = PANELS[n][0]
        dst = lg.at[(cls, (q, q_down, q_up, q_far)[way], *panel(n))]
        return send(l_own(n) if way == 0 else dst, dst, d_send.at[n, way], d_recv.at[n, way], col=q_twin)

    def part_a(n):
        if PANELS[n][0]:
            landed(l_own(n), t_recv.at[n])
        for way in range(2):
            l_copy(n, way).start()
        twin_copy(n, 0).start()

    def part_b(n):
        for way, owner in enumerate((q_down, q_up)):
            landed(lg.at[(PANELS[n][0], owner, *panel(n))], x_recv.at[n, way])
            l_copy(n, 2 + way).start()
        for way in range(2):
            twin_copy(n, 1 + way).start()

    def part_c(n):
        for way in range(2):
            landed(lg.at[(PANELS[n][0], q_far, *half_panel(n, way))], x_recv.at[n, 2 + way])
        twin_copy(n, 3).start()

    def part_d(n):
        for way, owner in enumerate((q, q_down, q_up, q_far)):
            twin = owner + 1 - 2 * lax.rem(owner, 2)
            landed(lg.at[(PANELS[n][0], twin, *panel(n))], d_recv.at[n, way])

    steps = {
        "p": functools.partial(own_b, 1), "m": functools.partial(own_b, 0), "f": relay_b,
        "t": lambda n: tri_copy(n).start(), "a": part_a, "b": part_b, "c": part_c,
    }

    def play(group, pos):
        for text in SCHEDULE.get((group, pos), ()):
            steps[text[0]](int(text[1:]))
        if pos == 0:
            for n, (_, first, _) in enumerate(PANELS):
                if first == group:
                    part_d(n)

    def events(j, pos, lo, hi):
        for group in range(lo, hi):
            if SCHEDULE.get((group, pos)) or (pos == 0 and any(p[1] == group for p in PANELS)):
                pl.when(j == group)(functools.partial(play, group, pos))

    def fetch_l(j, g, slot, wide):
        spot = rows_of(j), rows_of(g // 2)
        for p in range(4):
            owner = 4 * lax.rem(g, 2) + p
            dst = lbuf.at[slot, pl.ds(0, bs), pl.ds(p * bs, bs)]

            @pl.when(owner == q)
            def _():
                pltpu.make_async_copy(tri.at[spot], dst, lsem.at[slot]).start()

            @pl.when(owner != q)
            def _():
                pltpu.make_async_copy(lg.at[(0, owner, *spot)], dst, lsem.at[slot]).start()

            if not wide:
                dst = lbuf.at[slot, pl.ds(bs, bs), pl.ds(p * bs, bs)]
                pltpu.make_async_copy(lg.at[(1, owner, *spot)], dst, lsem.at[slot]).start()

    def fetch_block(owner, g, slot, wide, first=0, width=half):
        for side in range(2 if wide else 1):
            spot = rows_of(g), cols_of(side if wide else mine, first, width)
            dst = bbuf.at[slot, side, rows_of(owner), pl.ds(first, width)]

            @pl.when(owner == y)
            def _():
                pltpu.make_async_copy(rhs.at[spot], dst, bsem.at[slot]).start()

            @pl.when(owner != y)
            def _():
                pltpu.make_async_copy(bg.at[(owner, *spot)], dst, bsem.at[slot]).start()

    def fetch_b(g, slot, wide):
        for p in range(4):
            fetch_block(p, g, slot, wide)

    def l_fetched(slot, wide):
        landed(lbuf.at[slot, pl.ds(0, bs)] if wide else lbuf.at[slot], lsem.at[slot])

    def b_fetched(slot, wide):
        landed(bbuf.at[slot] if wide else bbuf.at[slot, 0], bsem.at[slot])

    tiles = half // tile

    def product(slot, n, wide):
        if wide:
            side, cols = n // tiles, pl.ds(pl.multiple_of(lax.rem(n, tiles) * tile, tile), tile)
            rows = rows_of(side)
            left = lbuf[slot, pl.ds(0, bs), :]
        else:
            side, cols = 0, pl.ds(pl.multiple_of(n * tile, tile), tile)
            rows = pl.ds(0, 2 * bs)
            left = lbuf[slot]
        term = jnp.dot(left, bbuf[slot, side, :, cols], preferred_element_type=jnp.float32)
        return rows, cols, acc[rows, cols] + term

    def multiply(slot, wide):
        @pl.loop(0, 2 * tiles if wide else tiles)
        def _(n):
            rows, cols, total = product(slot, n, wide)
            acc[rows, cols] = total

    def finish(j, slot, wide, lo=0, hi=tiles):
        @pl.loop(lo, 2 * tiles if wide else hi)
        def _(n):
            _, _, total = product(slot, n, wide)
            total = total.astype(out.dtype)
            if wide:
                out[rows_of(j), pl.ds(pl.multiple_of(n * tile, tile), tile)] = total
            else:
                cols = pl.ds(pl.multiple_of(n * tile, tile), tile)
                obuf[rows_of(j - NUM_WIDE), cols] = total[bs:]
                cols = pl.ds(pl.multiple_of(mine * half + n * tile, tile), tile)
                out[rows_of(j), cols] = total[:bs]

    def mate_copy(j, index, first=0, width=half):
        return send(obuf.at[rows_of(j - NUM_WIDE), pl.ds(first, width)],
                    out.at[rows_of(j), cols_of(mine, first, width)],
                    o_send.at[index], o_recv.at[index], row=mate)

    def older_terms(j, wide):
        def fetch(g):
            slot = lax.rem(g, SLOTS)

            @pl.when(g <= j)
            def _():
                fetch_l(j, g, slot, wide)

            @pl.when(g < j)
            def _():
                fetch_b(g, slot, wide)

        for g in range(SLOTS - 1):
            fetch(g)
        acc[...] = jnp.zeros_like(acc)

        @pl.loop(0, j)
        def _(g):
            slot = lax.rem(g, SLOTS)
            l_fetched(slot, wide)
            b_fetched(slot, wide)
            fetch(g + SLOTS - 1)
            multiply(slot, wide)

    def stage(j, wide, lo, hi):
        events(j, 0, lo, hi)
        older_terms(j, wide)
        events(j, 1, lo, hi)
        slot = lax.rem(j, SLOTS)
        fetch_block(y, j, slot, wide)
        fetch_block(mate, j, slot, wide)
        for kind, owner in ((1, peer), (2, far)):
            if wide:
                b_landed(kind, rows_of(j), cols_of(mine), 2 * j)
                b_landed(kind, rows_of(j), cols_of(1 - mine), 2 * j + 1)
            else:
                b_landed(kind, rows_of(j), cols_of(mine), NUM_WIDE + j)
            fetch_block(owner, j, slot, wide)
        l_fetched(slot, wide)
        b_fetched(slot, wide)
        finish(j, slot, wide)
        if not wide:
            mate_copy(j, j - NUM_WIDE).start()

    barrier = pltpu.get_barrier_semaphore()
    for where in ({"row": mate}, {"row": peer}, {"col": q_up}, {"col": q_down}, {"col": q_twin}):
        pl.semaphore_signal(barrier, inc=1, device_id=where, device_id_type=MESH)
    pl.semaphore_wait(barrier, 5)

    play(-1, 0)

    @pl.loop(0, NUM_WIDE)
    def _(j):
        stage(j, True, 0, NUM_WIDE)

    @pl.loop(NUM_WIDE, last)
    def _(j):
        stage(j, False, NUM_WIDE, last)

    play(last, 0)
    older_terms(last, False)
    play(last, 1)
    slot = last % SLOTS
    l_fetched(slot, False)
    for part in range(2):
        index, _, first, width = piece_of(last, part)
        fetch_block(y, last, slot, False, first, width)
        fetch_block(mate, last, slot, False, first, width)
        for kind, owner in ((1, peer), (2, far)):
            b_landed(kind, rows_of(last), cols_of(mine, first, width), index)
            fetch_block(owner, last, slot, False, first, width)
        landed(bbuf.at[slot, 0, :, pl.ds(first, width)], bsem.at[slot])
        finish(last, slot, False, part * tiles // 2, (part + 1) * tiles // 2)
        mate_copy(last, last - NUM_WIDE + part, first, width).start()

    for j in range(groups):
        for kind in range(3):
            for part in range(pieces(j)):
                b_copy(kind, j, part).wait_send()
    for n in range(len(PANELS)):
        if PANELS[n][0]:
            tri_copy(n).wait_send()
        for way in range(4):
            l_copy(n, way).wait_send()
            twin_copy(n, way).wait_send()

    @pl.loop(NUM_WIDE, last)
    def _(j):
        mate_copy(j, j - NUM_WIDE).wait_send()
        landed(out.at[rows_of(j), cols_of(1 - mine)], o_recv.at[j - NUM_WIDE])

    for part in range(2):
        index, _, first, width = piece_of(last, part)
        mate_copy(last, last - NUM_WIDE + part, first, width).wait_send()
        landed(out.at[rows_of(last), cols_of(1 - mine, first, width)], o_recv.at[last - NUM_WIDE + part])


def emit(parts, src, dst, sem):
    rows = src.shape[0] // parts

    def copy(n):
        spot = pl.ds(n * rows, rows)
        return pltpu.make_async_copy(src.at[spot], dst.at[spot], sem.at[n])

    for n in range(parts):
        copy(n).start()
    for n in range(parts):
        copy(n).wait()


def solution(mesh):
    grid_rows = mesh.shape["row"]
    grid_cols = mesh.shape["col"]
    bs = BLOCK_SIZE

    def local_trmm(tri_loc, rhs_loc):
        rows_loc, cols_loc = rhs_loc.shape
        groups = rows_loc // bs
        half = cols_loc // 2
        dtype = rhs_loc.dtype
        any_spec = pl.BlockSpec(memory_space=pl.ANY)
        vmem_spec = pl.BlockSpec(memory_space=pltpu.VMEM)
        dma = pltpu.SemaphoreType.DMA
        panels = len(PANELS)
        in_vmem, _, _ = pl.pallas_call(
            functools.partial(kernel, bs, min(TILE, half)),
            out_shape=[
                pltpu.VMEM((rows_loc, cols_loc), dtype),
                jax.ShapeDtypeStruct((grid_rows, rows_loc, cols_loc), dtype),
                jax.ShapeDtypeStruct((2, grid_cols, *tri_loc.shape), dtype),
            ],
            in_specs=[any_spec] * 2,
            out_specs=[vmem_spec, any_spec, any_spec],
            scratch_shapes=[
                pltpu.VMEM((SLOTS, 2 * bs, 4 * bs), dtype),
                pltpu.VMEM((SLOTS, 2, 4 * bs, half), dtype),
                pltpu.VMEM((2 * bs, half), jnp.float32),
                pltpu.VMEM(((groups - NUM_WIDE) * bs, half), dtype),
                dma((SLOTS,)), dma((SLOTS,)),
                dma((3, groups + NUM_WIDE + 1)), dma((3, groups + NUM_WIDE + 1)),
                dma((panels,)), dma((panels,)),
                dma((panels, 4)), dma((panels, 4)),
                dma((panels, 4)), dma((panels, 4)),
                dma((groups - NUM_WIDE + 1,)), dma((groups - NUM_WIDE + 1,)),
            ],
            compiler_params=pltpu.CompilerParams(
                collective_id=0, has_side_effects=True, vmem_limit_bytes=44 * 1024 * 1024),
        )(tri_loc, rhs_loc)
        return pl.pallas_call(
            functools.partial(emit, groups),
            out_shape=jax.ShapeDtypeStruct((rows_loc, cols_loc), dtype),
            in_specs=[vmem_spec],
            out_specs=any_spec,
            scratch_shapes=[dma((groups,))],
            compiler_params=pltpu.CompilerParams(vmem_limit_bytes=1024 * 1024),
        )(in_vmem)

    part_spec = P(("batch", "row"), "col")
    return jax.shard_map(local_trmm, mesh=mesh, in_specs=(part_spec, part_spec), out_specs=part_spec, check_vma=False)
```

```python
import functools

import jax
import jax.numpy as jnp
from jax import lax
from jax.experimental import pallas as pl
from jax.experimental.pallas import tpu as pltpu
from jax.sharding import PartitionSpec as P

BLOCK_SIZE = 256
TILE = 256
NUM_WIDE = 4
SLOTS = 4
MESH = pl.DeviceIdType.MESH

PANELS = (
    (0, 0, 2), (0, 2, 2), (0, 4, 2), (0, 6, 2), (1, 4, 2), (1, 6, 2), (0, 8, 2),
    (1, 8, 2), (0, 10, 1), (1, 10, 1), (0, 11, 1), (1, 11, 1),
)

SCHEDULE = {
    (-1, 0): ("t5", "m0", "p0", "t4", "a6", "p1", "a0", "a8",),
    (0, 0): ("b0", "a2", "p3", "f0", "c0",),
    (0, 1): ("a1", "m1", "b6", "m2", "t7", "b1", "p2", "m3",),
    (1, 0): ("p4", "a4", "b2", "a5", "f1", "c2", "m4",),
    (1, 1): ("f2", "a3",),
    (2, 0): ("m5", "b5", "f3", "c1", "p6", "m7", "t9",),
    (2, 1): ("b4", "f4", "b3", "c5", "m8",),
    (3, 0): ("c4", "m6", "f5", "a7", "p5",),
    (4, 1): ("b8", "m9",),
    (5, 0): ("f6", "t11", "c6", "p7", "b7", "c3",),
    (6, 0): ("f7", "a9",),
    (6, 1): ("p8", "f8",),
    (7, 0): ("a10", "m10", "c8", "c7",),
    (8, 0): ("f9", "b9",),
    (9, 0): ("p9", "a11", "c9",),
    (9, 1): ("m11", "f10", "b10",),
    (10, 0): ("b11", "p10",),
    (10, 1): ("p11", "c11", "c10", "f11",),
}


def kernel(bs, tile, tri, rhs, out, bg, lg, lbuf, bbuf, acc, obuf, lsem, bsem,
           b_send, b_recv, t_send, t_recv, x_send, x_recv, d_send, d_recv, o_send, o_recv):
    groups = rhs.shape[0] // bs
    last = groups - 1
    half = rhs.shape[1] // 2
    quarter = half // 2
    grid_rows = bg.shape[0]
    grid_cols = lg.shape[1]
    y = lax.axis_index("row")
    q = lax.axis_index("col")
    mate = y + 1 - 2 * lax.rem(y, 2)
    peer = grid_rows - 1 - y
    far = grid_rows - 1 - mate
    mine = lax.rem((y + 1) // 2 + 1, 2)
    q_up = lax.rem(q + 2, grid_cols)
    q_down = lax.rem(q + grid_cols - 2, grid_cols)
    q_far = lax.rem(q + grid_cols // 2, grid_cols)
    q_twin = q + 1 - 2 * lax.rem(q, 2)

    def send(src, dst, ss, rs, **where):
        return pltpu.make_async_remote_copy(src_ref=src, dst_ref=dst, send_sem=ss, recv_sem=rs,
                                            device_id=where, device_id_type=MESH)

    def landed(ref, sem):
        pltpu.make_async_copy(ref, ref, sem).wait()

    def rows_of(j, count=1):
        return pl.ds(pl.multiple_of(j * bs, bs), count * bs)

    def cols_of(side, first=0, width=half):
        return pl.ds(pl.multiple_of(side * half + first, width), width)

    def pieces(j):
        return 2 if j < NUM_WIDE or j == last else 1

    def piece_of(j, part):
        index = 2 * j + part if j < NUM_WIDE else NUM_WIDE + j + part
        if j == last:
            return index, False, part * quarter, quarter
        return index, part == 1, 0, half

    def b_copy(kind, j, part):
        index, other, first, width = piece_of(j, part)
        side = (mine if other else 1 - mine) if kind == 0 else (1 - mine if other else mine)
        spot = (rows_of(j), cols_of(side, first, width))
        src = bg.at[(mate, *spot)] if kind == 2 else rhs.at[spot]
        dst = bg.at[(mate if kind == 2 else y, *spot)]
        return send(src, dst, b_send.at[kind, index], b_recv.at[kind, index], row=mate if kind == 0 else peer)

    def b_landed(kind, rows, cols, index):
        landed(bg.at[(mate, peer, far)[kind], rows, cols], b_recv.at[kind, index])

    def own_b(kind, j):
        for part in range(pieces(j)):
            b_copy(kind, j, part).start()

    def relay_b(j):
        for part in range(pieces(j)):
            index, other, first, width = piece_of(j, part)
            b_landed(0, rows_of(j), cols_of(1 - mine if other else mine, first, width), index)
            b_copy(2, j, part).start()

    def panel(n):
        _, first, count = PANELS[n]
        return rows_of(first, count), pl.ds(0, ((first + count - 1) // 2 + 1) * bs)

    def half_panel(n, part):
        _, first, count = PANELS[n]
        rows = count * bs // 2
        start = pl.multiple_of(first * bs + part * rows, rows)
        return pl.ds(start, rows), pl.ds(0, ((first + count - 1) // 2 + 1) * bs)

    def tri_copy(n):
        return send(tri.at[panel(n)], lg.at[(1, q, *panel(n))], t_send.at[n], t_recv.at[n], row=mate)

    def l_own(n):
        return lg.at[(1, q, *panel(n))] if PANELS[n][0] else tri.at[panel(n)]

    def l_copy(n, way):
        cls = PANELS[n][0]
        sems = x_send.at[n, way], x_recv.at[n, way]
        where = q_up if way in (0, 2) else q_down
        if way < 2:
            return send(l_own(n), lg.at[(cls, q, *panel(n))], *sems, col=where)
        part = lg.at[(cls, q_down if way == 2 else q_up, *half_panel(n, way - 2))]
        return send(part, part, *sems, col=where)

    def twin_copy(n, way):
        cls = PANELS[n][0]
        dst = lg.at[(cls, (q, q_down, q_up, q_far)[way], *panel(n))]
        return send(l_own(n) if way == 0 else dst, dst, d_send.at[n, way], d_recv.at[n, way], col=q_twin)

    def part_a(n):
        if PANELS[n][0]:
            landed(l_own(n), t_recv.at[n])
        for way in range(2):
            l_copy(n, way).start()
        twin_copy(n, 0).start()

    def part_b(n):
        for way, owner in enumerate((q_down, q_up)):
            landed(lg.at[(PANELS[n][0], owner, *panel(n))], x_recv.at[n, way])
            l_copy(n, 2 + way).start()
        for way in range(2):
            twin_copy(n, 1 + way).start()

    def part_c(n):
        for way in range(2):
            landed(lg.at[(PANELS[n][0], q_far, *half_panel(n, way))], x_recv.at[n, 2 + way])
        twin_copy(n, 3).start()

    def part_d(n):
        for way, owner in enumerate((q, q_down, q_up, q_far)):
            twin = owner + 1 - 2 * lax.rem(owner, 2)
            landed(lg.at[(PANELS[n][0], twin, *panel(n))], d_recv.at[n, way])

    steps = {
        "p": functools.partial(own_b, 1), "m": functools.partial(own_b, 0), "f": relay_b,
        "t": lambda n: tri_copy(n).start(), "a": part_a, "b": part_b, "c": part_c,
    }

    def play(group, pos):
        for text in SCHEDULE.get((group, pos), ()):
            steps[text[0]](int(text[1:]))
        if pos == 0:
            for n, (_, first, _) in enumerate(PANELS):
                if first == group:
                    part_d(n)

    def events(j, pos, lo, hi):
        for group in range(lo, hi):
            if SCHEDULE.get((group, pos)) or (pos == 0 and any(p[1] == group for p in PANELS)):
                pl.when(j == group)(functools.partial(play, group, pos))

    def fetch_l(j, g, slot, wide):
        spot = rows_of(j), rows_of(g // 2)
        for p in range(4):
            owner = 4 * lax.rem(g, 2) + p
            dst = lbuf.at[slot, pl.ds(0, bs), pl.ds(p * bs, bs)]

            @pl.when(owner == q)
            def _():
                pltpu.make_async_copy(tri.at[spot], dst, lsem.at[slot]).start()

            @pl.when(owner != q)
            def _():
                pltpu.make_async_copy(lg.at[(0, owner, *spot)], dst, lsem.at[slot]).start()

            if not wide:
                dst = lbuf.at[slot, pl.ds(bs, bs), pl.ds(p * bs, bs)]
                pltpu.make_async_copy(lg.at[(1, owner, *spot)], dst, lsem.at[slot]).start()

    def fetch_block(owner, g, slot, wide, first=0, width=half):
        for side in range(2 if wide else 1):
            spot = rows_of(g), cols_of(side if wide else mine, first, width)
            dst = bbuf.at[slot, side, rows_of(owner), pl.ds(first, width)]

            @pl.when(owner == y)
            def _():
                pltpu.make_async_copy(rhs.at[spot], dst, bsem.at[slot]).start()

            @pl.when(owner != y)
            def _():
                pltpu.make_async_copy(bg.at[(owner, *spot)], dst, bsem.at[slot]).start()

    def fetch_b(g, slot, wide):
        for p in range(4):
            fetch_block(p, g, slot, wide)

    def l_fetched(slot, wide):
        landed(lbuf.at[slot, pl.ds(0, bs)] if wide else lbuf.at[slot], lsem.at[slot])

    def b_fetched(slot, wide):
        landed(bbuf.at[slot] if wide else bbuf.at[slot, 0], bsem.at[slot])

    tiles = half // tile

    def product(slot, n, wide):
        if wide:
            side, cols = n // tiles, pl.ds(pl.multiple_of(lax.rem(n, tiles) * tile, tile), tile)
            rows = rows_of(side)
            left = lbuf[slot, pl.ds(0, bs), :]
        else:
            side, cols = 0, pl.ds(pl.multiple_of(n * tile, tile), tile)
            rows = pl.ds(0, 2 * bs)
            left = lbuf[slot]
        term = jnp.dot(left, bbuf[slot, side, :, cols], preferred_element_type=jnp.float32)
        return rows, cols, acc[rows, cols] + term

    def multiply(slot, wide):
        @pl.loop(0, 2 * tiles if wide else tiles)
        def _(n):
            rows, cols, total = product(slot, n, wide)
            acc[rows, cols] = total

    def finish(j, slot, wide, lo=0, hi=tiles):
        @pl.loop(lo, 2 * tiles if wide else hi)
        def _(n):
            _, _, total = product(slot, n, wide)
            total = total.astype(out.dtype)
            if wide:
                out[rows_of(j), pl.ds(pl.multiple_of(n * tile, tile), tile)] = total
            else:
                cols = pl.ds(pl.multiple_of(n * tile, tile), tile)
                obuf[rows_of(j - NUM_WIDE), cols] = total[bs:]
                cols = pl.ds(pl.multiple_of(mine * half + n * tile, tile), tile)
                out[rows_of(j), cols] = total[:bs]

    def mate_copy(j, index, first=0, width=half):
        return send(obuf.at[rows_of(j - NUM_WIDE), pl.ds(first, width)],
                    out.at[rows_of(j), cols_of(mine, first, width)],
                    o_send.at[index], o_recv.at[index], row=mate)

    def older_terms(j, wide):
        def fetch(g):
            slot = lax.rem(g, SLOTS)

            @pl.when(g <= j)
            def _():
                fetch_l(j, g, slot, wide)

            @pl.when(g < j)
            def _():
                fetch_b(g, slot, wide)

        for g in range(SLOTS - 1):
            fetch(g)
        acc[...] = jnp.zeros_like(acc)

        @pl.loop(0, j)
        def _(g):
            slot = lax.rem(g, SLOTS)
            l_fetched(slot, wide)
            b_fetched(slot, wide)
            fetch(g + SLOTS - 1)
            multiply(slot, wide)

    def stage(j, wide, lo, hi):
        events(j, 0, lo, hi)
        older_terms(j, wide)
        events(j, 1, lo, hi)
        slot = lax.rem(j, SLOTS)
        fetch_block(y, j, slot, wide)
        fetch_block(mate, j, slot, wide)
        for kind, owner in ((1, peer), (2, far)):
            if wide:
                b_landed(kind, rows_of(j), cols_of(mine), 2 * j)
                b_landed(kind, rows_of(j), cols_of(1 - mine), 2 * j + 1)
            else:
                b_landed(kind, rows_of(j), cols_of(mine), NUM_WIDE + j)
            fetch_block(owner, j, slot, wide)
        l_fetched(slot, wide)
        b_fetched(slot, wide)
        finish(j, slot, wide)
        if not wide:
            mate_copy(j, j - NUM_WIDE).start()

    barrier = pltpu.get_barrier_semaphore()
    for where in ({"row": mate}, {"row": peer}, {"col": q_up}, {"col": q_down}, {"col": q_twin}):
        pl.semaphore_signal(barrier, inc=1, device_id=where, device_id_type=MESH)
    pl.semaphore_wait(barrier, 5)

    play(-1, 0)

    @pl.loop(0, NUM_WIDE)
    def _(j):
        stage(j, True, 0, NUM_WIDE)

    @pl.loop(NUM_WIDE, last)
    def _(j):
        stage(j, False, NUM_WIDE, last)

    play(last, 0)
    older_terms(last, False)
    play(last, 1)
    slot = last % SLOTS
    l_fetched(slot, False)
    for part in range(2):
        index, _, first, width = piece_of(last, part)
        fetch_block(y, last, slot, False, first, width)
        fetch_block(mate, last, slot, False, first, width)
        for kind, owner in ((1, peer), (2, far)):
            b_landed(kind, rows_of(last), cols_of(mine, first, width), index)
            fetch_block(owner, last, slot, False, first, width)
        landed(bbuf.at[slot, 0, :, pl.ds(first, width)], bsem.at[slot])
        finish(last, slot, False, part * tiles // 2, (part + 1) * tiles // 2)
        mate_copy(last, last - NUM_WIDE + part, first, width).start()

    for j in range(groups):
        for kind in range(3):
            for part in range(pieces(j)):
                b_copy(kind, j, part).wait_send()
    for n in range(len(PANELS)):
        if PANELS[n][0]:
            tri_copy(n).wait_send()
        for way in range(4):
            l_copy(n, way).wait_send()
            twin_copy(n, way).wait_send()

    @pl.loop(NUM_WIDE, last)
    def _(j):
        mate_copy(j, j - NUM_WIDE).wait_send()
        landed(out.at[rows_of(j), cols_of(1 - mine)], o_recv.at[j - NUM_WIDE])

    for part in range(2):
        index, _, first, width = piece_of(last, part)
        mate_copy(last, last - NUM_WIDE + part, first, width).wait_send()
        landed(out.at[rows_of(last), cols_of(1 - mine, first, width)], o_recv.at[last - NUM_WIDE + part])


def emit(parts, src, dst, sem):
    rows = src.shape[0] // parts

    def copy(n):
        spot = pl.ds(n * rows, rows)
        return pltpu.make_async_copy(src.at[spot], dst.at[spot], sem.at[n])

    for n in range(parts):
        copy(n).start()
    for n in range(parts):
        copy(n).wait()


def solution(mesh):
    grid_rows = mesh.shape["row"]
    grid_cols = mesh.shape["col"]
    bs = BLOCK_SIZE

    def local_trmm(tri_loc, rhs_loc):
        rows_loc, cols_loc = rhs_loc.shape
        groups = rows_loc // bs
        half = cols_loc // 2
        dtype = rhs_loc.dtype
        any_spec = pl.BlockSpec(memory_space=pl.ANY)
        vmem_spec = pl.BlockSpec(memory_space=pltpu.VMEM)
        dma = pltpu.SemaphoreType.DMA
        panels = len(PANELS)
        in_vmem, _, _ = pl.pallas_call(
            functools.partial(kernel, bs, min(TILE, half)),
            out_shape=[
                pltpu.VMEM((rows_loc, cols_loc), dtype),
                jax.ShapeDtypeStruct((grid_rows, rows_loc, cols_loc), dtype),
                jax.ShapeDtypeStruct((2, grid_cols, *tri_loc.shape), dtype),
            ],
            in_specs=[any_spec] * 2,
            out_specs=[vmem_spec, any_spec, any_spec],
            scratch_shapes=[
                pltpu.VMEM((SLOTS, 2 * bs, 4 * bs), dtype),
                pltpu.VMEM((SLOTS, 2, 4 * bs, half), dtype),
                pltpu.VMEM((2 * bs, half), jnp.float32),
                pltpu.VMEM(((groups - NUM_WIDE) * bs, half), dtype),
                dma((SLOTS,)), dma((SLOTS,)),
                dma((3, groups + NUM_WIDE + 1)), dma((3, groups + NUM_WIDE + 1)),
                dma((panels,)), dma((panels,)),
                dma((panels, 4)), dma((panels, 4)),
                dma((panels, 4)), dma((panels, 4)),
                dma((groups - NUM_WIDE + 1,)), dma((groups - NUM_WIDE + 1,)),
            ],
            compiler_params=pltpu.CompilerParams(
                collective_id=0, has_side_effects=True, vmem_limit_bytes=44 * 1024 * 1024),
        )(tri_loc, rhs_loc)
        return pl.pallas_call(
            functools.partial(emit, groups),
            out_shape=jax.ShapeDtypeStruct((rows_loc, cols_loc), dtype),
            in_specs=[vmem_spec],
            out_specs=any_spec,
            scratch_shapes=[dma((groups,))],
            compiler_params=pltpu.CompilerParams(vmem_limit_bytes=1024 * 1024),
        )(in_vmem)

    part_spec = P(("batch", "row"), "col")
    return jax.shard_map(local_trmm, mesh=mesh, in_specs=(part_spec, part_spec), out_specs=part_spec, check_vma=False)
```
